128 devices in a mesh: row: 16 (over y, z), col: 8 (over x, core).
Axes of the slice: x: 4, y: 4, z: 4, core: 2. Of those that a mesh axis runs over, the one named last changes fastest.
Arguments:
- densities: bfloat16 [18432, 3072], P(('row', 'col')), may hold values from -0.796875 to 0.796875
- counts: int32 [2048], P(('row', 'col')), may hold values from 3 to 9
- coulomb: float32 [3072], replicated, may hold values from 0.05 to 1
- energies: float32 [18432], P(('row', 'col')), may hold values from 8 to 64
- vectors: bfloat16 [18432, 64], P(('row', 'col')), may hold values from -0.046875 to 0.046875
Outputs:
- kernel: float32 [18432, 18432], P('row', 'col')
- product: float32 [18432, 64], P(('row', 'col'))
The draws below stay inside these ranges and needn't reach their ends.
All inputs are finite; a program needn't handle non-finite values.
Results may differ from the reference program's by a relative error of at most 0.0095.
Values may be sent and summed in bfloat16 or wider, within the bound.
No kernel may reach another device: no remote copies, remote signals or barrier semaphores. Data moves between devices by JAX's collectives and lax.ppermute only.
A program may use at most 128 MiB of HBM per device.

```python
import math
import jax
import jax.numpy as jnp
from jax import lax

G = 3072
NV = 64
SLOT = 9
K_DEV = 16
NK = 2048
ROWS = 18432
N_ROW = 16
N_COL = 8


def set_ends(values, own_key, low, largest):
    spot = [jax.random.randint(jax.random.fold_in(own_key, axis), (), 0, length) for axis, length in enumerate(values.shape)]
    main_axis = values.shape.index(max(values.shape))
    beside = spot[:main_axis] + [(spot[main_axis] + 1) % values.shape[main_axis]] + spot[main_axis + 1:]
    return values.at[tuple(spot)].set(low).at[tuple(beside)].set(largest)


def levels(rng, shape, split, smallest, high):
    def one(position, shards_of):
        heights = jax.random.uniform(jax.random.fold_in(jax.random.fold_in(rng, 6), position), (shards_of,), jnp.float32, smallest / len(split), high / len(split))
        return jnp.repeat(jnp.exp(heights), shape[position] // shards_of).reshape((-1,) + (1,) * (len(shape) - position - 1))

    gain = one(*split[0])
    for cut in split[1:]:
        gain = gain * one(*cut)
    return gain


def noise(rng, dims, deviation, reach, shards=(), dtype=jnp.bfloat16):
    array = deviation * jax.random.normal(rng, dims, jnp.float32)
    if shards:
        array = array * levels(rng, dims, shards, -0.22, 0.18)
    return jnp.clip(array, -reach, reach).astype(dtype)


def setup_inputs(seed: int = 0) -> dict:
    seeds = jax.random.split(jax.random.key(seed), 6)
    densities = noise(seeds[0], (ROWS, G), 0.134, 0.796875, ((0, 128),))
    counts = set_ends(jax.random.randint(seeds[1], (NK,), 3, 10), jax.random.fold_in(seeds[1], 1), 3, 9).astype(jnp.int32)
    coulomb = jnp.clip(jnp.exp(jax.random.uniform(seeds[2], (G,), jnp.float32, math.log(0.05), math.log(1.0))), 0.05, 1.0)
    energies = jnp.clip(jnp.exp(math.log(64.0) - 2.0794415 * jax.random.uniform(seeds[3], (ROWS,), jnp.float32) ** levels(seeds[3], (ROWS,), ((0, 128),), -0.2, 0.2)), 8.0, 64.0)
    vectors = noise(seeds[4], (ROWS, NV), ROWS ** -0.5, 0.046875, ((0, 128),))
    return {"densities": densities, "counts": counts, "coulomb": coulomb, "energies": energies, "vectors": vectors}


def reference(densities, counts, coulomb, energies, vectors):
    slots_idx = lax.broadcasted_iota(jnp.int32, (NK, SLOT), 1)
    usable = (slots_idx < counts[:, None]).reshape(NK * SLOT)
    masked = jnp.where(usable[:, None], densities.astype(jnp.float32), 0.0)
    weighted = lax.optimization_barrier((masked * coulomb[None, :]).astype(jnp.bfloat16)).astype(jnp.float32)
    ordered = masked.reshape(N_ROW, N_COL, K_DEV * SLOT, G).transpose(1, 0, 2, 3).reshape(NK * SLOT, G)
    kernel = jnp.dot(weighted, ordered.T, precision=lax.Precision.HIGHEST, preferred_element_type=jnp.float32)
    projected = jnp.dot(masked.T, vectors.astype(jnp.float32), precision=lax.Precision.HIGHEST, preferred_element_type=jnp.float32)
    coupled = jnp.dot(weighted, projected, precision=lax.Precision.HIGHEST, preferred_element_type=jnp.float32)
    diagonal = jnp.where(usable, energies, 0.0)
    product = coupled + diagonal[:, None] * vectors.astype(jnp.float32)
    return kernel, product
```

```python
import functools

import jax
import jax.numpy as jnp
from jax import lax
from jax.experimental import pallas as pl
from jax.experimental.pallas import tpu as pltpu
from jax.sharding import Mesh
from jax.sharding import PartitionSpec as P

SLOT = 9
LANES = 128
WINDOW = 256
MESH_AXES = ("y", "z", "x", "core")
PLANE = ("y", "z", "core")
VMEM = pl.BlockSpec(memory_space=pltpu.VMEM)
SMEM = pl.BlockSpec(memory_space=pltpu.SMEM)
ANY = pl.BlockSpec(memory_space=pl.ANY)


def plane_perm(sizes, phase, step):
    ny, nz, nc = sizes
    pairs = []
    for y in range(ny):
        for z in range(nz):
            for core in range(nc):
                if (core == 0) == (phase == 1):
                    to = ((y + step) % ny, z)
                else:
                    to = (y, (z + step) % nz)
                pairs.append(((y * nz + z) * nc + core, (to[0] * nz + to[1]) * nc + core))
    return pairs


def in_plane(value, phase, step):
    sizes = tuple(lax.axis_size(name) for name in PLANE)
    return lax.ppermute(value, PLANE, plane_perm(sizes, phase, step))


def along_x(value, step):
    size = lax.axis_size("x")
    return lax.ppermute(value, "x", [(i, (i + step) % size) for i in range(size)])


def rows_body(*refs):
    place, blocks, out, sems = refs[0], refs[1:-2], refs[-2], refs[-1]
    copies = []
    for ref in blocks:
        for j in range(ref.shape[0]):
            at = len(copies)
            block = ref.shape[1]
            start = pl.multiple_of(place[at] * block, 16)
            copies.append(pltpu.make_async_copy(ref.at[j], out.at[pl.ds(start, block)], sems.at[at]))
            copies[-1].start()
    for copy in copies:
        copy.wait()


def stacked_rows(place, blocks):
    count = sum(value.shape[0] for value in blocks)
    block, width = blocks[0].shape[1:]
    return pl.pallas_call(
        rows_body,
        out_shape=pltpu.VMEM((count * block, width), jnp.bfloat16),
        in_specs=[SMEM] + [ANY] * len(blocks),
        out_specs=VMEM,
        scratch_shapes=[pltpu.SemaphoreType.DMA((count,))],
        compiler_params=pltpu.CompilerParams(vmem_limit_bytes=12 << 20),
        cost_estimate=pl.CostEstimate(flops=2 * 10**9, bytes_accessed=4 * count * block * width, transcendentals=0),
        name="rows",
    )(place, *blocks)


def tile_body(counts, first, last, step, *refs):
    count, block = sum(counts), refs[2].shape[1]
    place, rows, vectors = refs[:3]
    blocks, rest = refs[3 : 3 + len(counts)], refs[3 + len(counts) :]
    if not first:
        rest = rest[2:]
    tile, partial = rest[:2]
    rest = rest[2:]
    if last:
        result, rest = rest[0], rest[1:]
    held, held_vectors, sems = rest[:3]
    copies = []
    for ref, number in zip(blocks, counts):
        for j in range(number):
            at = len(copies)
            source = ref.at[j] if len(ref.shape) == 3 else ref
            copies.append(pltpu.make_async_copy(source, held.at[pl.ds(at * block, block)], sems.at[at]))
            copies[-1].start()
    if held.shape[0] > count * block:
        held[count * block :, :] = jnp.zeros((held.shape[0] - count * block, held.shape[1]), held.dtype)
    held_vectors[...] = jnp.zeros(held_vectors.shape, held_vectors.dtype)
    for at in range(count):
        held_vectors[pl.ds(at * block, block), :] = vectors[place[at]]
    for copy in copies:
        copy.wait()
    lane = lax.broadcasted_iota(jnp.int32, (step, WINDOW), 1)

    def chunk(number, carry):
        part = pl.ds(pl.multiple_of(number * step, step), step)
        values = lax.dot_general(
            rows[part, :], held[...], (((1,), (1,)), ((), ())), preferred_element_type=jnp.float32
        )
        share = jnp.dot(values.astype(jnp.bfloat16), held_vectors[...], preferred_element_type=jnp.float32)
        partial[part, :] = share if first else partial[part, :] + share
        for at in range(count):
            source = at * block // LANES * LANES
            start = place[at] * block
            base = pl.multiple_of(start // LANES * LANES, LANES)
            shift = start - base
            moved = pltpu.roll(values[:, source : source + WINDOW], lax.rem(shift + source - at * block + WINDOW, WINDOW), 1)
            keep = (lane >= shift) & (lane < shift + block)
            window = (part, pl.ds(base, WINDOW))
            tile[window] = jnp.where(keep, moved, tile[window])
        if last:
            pltpu.make_async_copy(tile.at[part], result.at[part], rest[3]).start()
        return carry

    lax.fori_loop(0, rows.shape[0] // step, chunk, 0)
    if last:
        pltpu.make_async_copy(tile, result, rest[3]).wait()


def into_tile(place, rows, vectors, blocks, state, columns, last=False):
    counts = [value.shape[0] if value.ndim == 3 else 1 for value in blocks]
    count, (block, width) = sum(counts), blocks[0].shape[-2:]
    padded = max(-(-count * block // LANES) * LANES, (count - 1) * block // LANES * LANES + WINDOW)
    height, wide = rows.shape[0], vectors.shape[-1]
    first = state is None
    step = height // 3 if last else height
    shapes = [pltpu.VMEM((height, columns), jnp.float32), pltpu.VMEM((height, wide), jnp.float32)]
    scratch = [
        pltpu.VMEM((padded, width), jnp.bfloat16),
        pltpu.VMEM((padded, wide), jnp.bfloat16),
        pltpu.SemaphoreType.DMA((count,)),
    ]
    if last:
        shapes.append(jax.ShapeDtypeStruct((height, columns), jnp.float32))
        scratch.append(pltpu.SemaphoreType.DMA)
    operands = [place, rows, vectors, *blocks] + ([] if first else list(state))
    return pl.pallas_call(
        functools.partial(tile_body, counts, first, last, step),
        out_shape=shapes,
        in_specs=[SMEM, VMEM, VMEM] + [ANY] * len(blocks) + ([] if first else [VMEM, VMEM]),
        out_specs=[VMEM, VMEM] + ([ANY] if last else []),
        input_output_aliases={} if first else {len(operands) - 2: 0, len(operands) - 1: 1},
        scratch_shapes=scratch,
        compiler_params=pltpu.CompilerParams(vmem_limit_bytes=28 << 20),
        cost_estimate=pl.CostEstimate(
            flops=2 * height * padded * width, bytes_accessed=2 * count * block * width, transcendentals=0
        ),
        name=f"tile_{count}",
    )(*operands)


def body(densities, counts, coulomb, energies, vectors):
    kpoints = counts.shape[0]
    slot_index = lax.broadcasted_iota(jnp.int32, (kpoints, SLOT), 1)
    usable = (slot_index < counts[:, None]).reshape(kpoints * SLOT)
    masked = jnp.where(usable[:, None], densities, jnp.zeros_like(densities))
    weighted = (masked.astype(jnp.float32) * coulomb[None, :]).astype(jnp.bfloat16)
    block, width = masked.shape
    half = width // 2
    ny, nz, nx, nc = (lax.axis_size(name) for name in MESH_AXES)
    y, z, x, core = (lax.axis_index(name) for name in MESH_AXES)

    own_up, own_down = in_plane(masked, 2, 1), in_plane(masked, 2, -1)
    up, down = in_plane(masked, 1, 1), in_plane(masked, 1, -1)
    far = jnp.concatenate([in_plane(up[:, :half], 1, 1), in_plane(down[:, half:], 1, -1)], axis=1)
    near = jnp.stack([up, down])
    near_up, near_down = in_plane(near, 2, 1), in_plane(near, 2, -1)
    far_up, far_down = in_plane(far, 2, 1), in_plane(far, 2, -1)
    own_far = in_plane(own_down, 2, -1)
    near_far = in_plane(near_up, 2, 1)
    far_far = in_plane(far_down, 2, -1)

    ring = jnp.stack([weighted, along_x(weighted, 1), along_x(weighted, -1), along_x(weighted, 2)])
    other = lax.ppermute(ring, "core", [(i, (i + 1) % nc) for i in range(nc)])
    x_at = (x - jnp.array([0, 1, -1, 2], jnp.int32)) % nx
    row_place = jnp.concatenate([x_at * nc + core, x_at * nc + (nc - 1 - core)])
    rows = stacked_rows(row_place, [ring, other])

    copies = jnp.broadcast_to(vectors[None], (ny * nz, *vectors.shape))
    column_vectors = lax.all_to_all(copies, ("y", "z"), 0, 0, tiled=True)

    def place(*offsets):
        steps = jnp.array(offsets, jnp.int32)
        along_y = (y - jnp.where(core == 0, steps[:, 0], steps[:, 1])) % ny
        along_z = (z - jnp.where(core == 0, steps[:, 1], steps[:, 0])) % nz
        return along_y * nz + along_z

    columns = ny * nz * block
    fill = functools.partial(into_tile, rows=rows, vectors=column_vectors, columns=columns)
    state = fill(place((0, 0), (1, 0), (-1, 0), (2, 0)), blocks=[masked, up, down, far], state=None)
    state = fill(place((0, 1), (0, -1), (0, 2)), blocks=[own_up, own_down, own_far], state=state)
    state = fill(place((1, 1), (-1, 1), (2, 1)), blocks=[near_up, far_up], state=state)
    state = fill(place((1, -1), (-1, -1), (2, -1)), blocks=[near_down, far_down], state=state)
    _, partial, kernel = fill(place((1, 2), (-1, 2), (2, 2)), blocks=[near_far, far_far], state=state, last=True)

    shares = partial.astype(jnp.bfloat16).reshape(nx * nc, block, -1)
    shares = lax.all_to_all(shares, ("x", "core"), 0, 0, tiled=True)
    coupled = jnp.sum(shares.astype(jnp.float32), axis=0)
    diagonal = jnp.where(usable, energies, jnp.zeros_like(energies))
    product = coupled + diagonal[:, None] * vectors.astype(jnp.float32)
    return (kernel, product)


def solution(mesh):
    ny, nz = 4, mesh.shape["row"] // 4
    nx, nc = mesh.shape["col"] // 2, 2
    finer = Mesh(mesh.devices.reshape(ny, nz, nx, nc), MESH_AXES)
    in_specs = (P(MESH_AXES, None), P(MESH_AXES), P(), P(MESH_AXES), P(MESH_AXES, None))
    out_specs = (P(("y", "z"), ("x", "core")), P(MESH_AXES, None))
    return jax.shard_map(body, mesh=finer, in_specs=in_specs, out_specs=out_specs, check_vma=False)
```

```python
import functools

import jax
import jax.numpy as jnp
from jax import lax
from jax.experimental import pallas as pl
from jax.experimental.pallas import tpu as pltpu
from jax.sharding import Mesh
from jax.sharding import PartitionSpec as P

SLOT = 9
LANES = 128
WINDOW = 256
MESH_AXES = ("y", "z", "x", "core")
PLANE = ("y", "z", "core")
VMEM = pl.BlockSpec(memory_space=pltpu.VMEM)
SMEM = pl.BlockSpec(memory_space=pltpu.SMEM)
ANY = pl.BlockSpec(memory_space=pl.ANY)


def plane_perm(sizes, phase, step):
    ny, nz, nc = sizes
    pairs = []
    for y in range(ny):
        for z in range(nz):
            for core in range(nc):
                if (core == 0) == (phase == 1):
                    to = ((y + step) % ny, z)
                else:
                    to = (y, (z + step) % nz)
                pairs.append(((y * nz + z) * nc + core, (to[0] * nz + to[1]) * nc + core))
    return pairs


def in_plane(value, phase, step):
    sizes = tuple(lax.axis_size(axis) for axis in PLANE)
    return lax.ppermute(value, PLANE, plane_perm(sizes, phase, step))


def along_x(value, step):
    size = lax.axis_size("x")
    return lax.ppermute(value, "x", [(i, (i + step) % size) for i in range(size)])


def rows_body(*refs):
    place, blocks, out, sems = refs[0], refs[1:-2], refs[-2], refs[-1]
    copies = []
    for ref in blocks:
        for j in range(ref.shape[0]):
            at = len(copies)
            block = ref.shape[1]
            start = pl.multiple_of(place[at] * block, 16)
            copies.append(pltpu.make_async_copy(ref.at[j], out.at[pl.ds(start, block)], sems.at[at]))
            copies[-1].start()
    for copy in copies:
        copy.wait()


def stacked_rows(place, blocks):
    count = sum(value.shape[0] for value in blocks)
    block, width = blocks[0].shape[1:]
    return pl.pallas_call(
        rows_body,
        out_shape=pltpu.VMEM((count * block, width), jnp.bfloat16),
        in_specs=[SMEM] + [ANY] * len(blocks),
        out_specs=VMEM,
        scratch_shapes=[pltpu.SemaphoreType.DMA((count,))],
        compiler_params=pltpu.CompilerParams(vmem_limit_bytes=12 << 20),
        cost_estimate=pl.CostEstimate(flops=2 * 10**9, bytes_accessed=4 * count * block * width, transcendentals=0),
        name="rows",
    )(place, *blocks)


def tile_body(counts, first, last, step, *refs):
    count, block = sum(counts), refs[2].shape[1]
    place, rows, vectors = refs[:3]
    blocks, rest = refs[3 : 3 + len(counts)], refs[3 + len(counts) :]
    if not first:
        rest = rest[2:]
    tile, partial = rest[:2]
    rest = rest[2:]
    if last:
        result, rest = rest[0], rest[1:]
    held, held_vectors, sems = rest[:3]
    copies = []
    for ref, number in zip(blocks, counts):
        for j in range(number):
            at = len(copies)
            source = ref.at[j] if len(ref.shape) == 3 else ref
            copies.append(pltpu.make_async_copy(source, held.at[pl.ds(at * block, block)], sems.at[at]))
            copies[-1].start()
    if held.shape[0] > count * block:
        held[count * block :, :] = jnp.zeros((held.shape[0] - count * block, held.shape[1]), held.dtype)
    held_vectors[...] = jnp.zeros(held_vectors.shape, held_vectors.dtype)
    for at in range(count):
        held_vectors[pl.ds(at * block, block), :] = vectors[place[at]]
    for copy in copies:
        copy.wait()
    lane = lax.broadcasted_iota(jnp.int32, (step, WINDOW), 1)

    def chunk(number, carry):
        part = pl.ds(pl.multiple_of(number * step, step), step)
        values = lax.dot_general(
            rows[part, :], held[...], (((1,), (1,)), ((), ())), preferred_element_type=jnp.float32
        )
        share = jnp.dot(values.astype(jnp.bfloat16), held_vectors[...], preferred_element_type=jnp.float32)
        partial[part, :] = share if first else partial[part, :] + share
        for at in range(count):
            source = at * block // LANES * LANES
            start = place[at] * block
            base = pl.multiple_of(start // LANES * LANES, LANES)
            shift = start - base
            moved = pltpu.roll(values[:, source : source + WINDOW], lax.rem(shift + source - at * block + WINDOW, WINDOW), 1)
            keep = (lane >= shift) & (lane < shift + block)
            window = (part, pl.ds(base, WINDOW))
            tile[window] = jnp.where(keep, moved, tile[window])
        if last:
            pltpu.make_async_copy(tile.at[part], result.at[part], rest[3]).start()
        return carry

    lax.fori_loop(0, rows.shape[0] // step, chunk, 0)
    if last:
        pltpu.make_async_copy(tile, result, rest[3]).wait()


def into_tile(place, rows, vectors, blocks, state, columns, last=False):
    counts = [value.shape[0] if value.ndim == 3 else 1 for value in blocks]
    count, (block, width) = sum(counts), blocks[0].shape[-2:]
    padded = max(-(-count * block // LANES) * LANES, (count - 1) * block // LANES * LANES + WINDOW)
    height, wide = rows.shape[0], vectors.shape[-1]
    first = state is None
    step = height // 3 if last else height
    shapes = [pltpu.VMEM((height, columns), jnp.float32), pltpu.VMEM((height, wide), jnp.float32)]
    scratch = [
        pltpu.VMEM((padded, width), jnp.bfloat16),
        pltpu.VMEM((padded, wide), jnp.bfloat16),
        pltpu.SemaphoreType.DMA((count,)),
    ]
    if last:
        shapes.append(jax.ShapeDtypeStruct((height, columns), jnp.float32))
        scratch.append(pltpu.SemaphoreType.DMA)
    operands = [place, rows, vectors, *blocks] + ([] if first else list(state))
    return pl.pallas_call(
        functools.partial(tile_body, counts, first, last, step),
        out_shape=shapes,
        in_specs=[SMEM, VMEM, VMEM] + [ANY] * len(blocks) + ([] if first else [VMEM, VMEM]),
        out_specs=[VMEM, VMEM] + ([ANY] if last else []),
        input_output_aliases={} if first else {len(operands) - 2: 0, len(operands) - 1: 1},
        scratch_shapes=scratch,
        compiler_params=pltpu.CompilerParams(vmem_limit_bytes=16 << 20),
        cost_estimate=pl.CostEstimate(
            flops=2 * height * padded * width, bytes_accessed=2 * count * block * width, transcendentals=0
        ),
    )(*operands)


def work(densities, counts, coulomb, energies, vectors):
    kpoints = counts.shape[0]
    slot_index = lax.broadcasted_iota(jnp.int32, (kpoints, SLOT), 1)
    usable = (slot_index < counts[:, None]).reshape(kpoints * SLOT)
    masked = jnp.where(usable[:, None], densities, jnp.zeros_like(densities))
    weighted = (masked.astype(jnp.float32) * coulomb[None, :]).astype(jnp.bfloat16)
    block, _ = masked.shape
    ny, nz, nx, nc = (lax.axis_size(name) for name in MESH_AXES)
    y, z, x, core = (lax.axis_index(name) for name in MESH_AXES)

    up, down, far = (in_plane(masked, 1, step) for step in (1, -1, 2))
    low, high = jnp.stack([masked, up]), jnp.stack([down, far])
    low_up, high_down = in_plane(low, 2, 1), in_plane(high, 2, -1)
    high_up, low_down = in_plane(high, 2, 1), in_plane(low, 2, -1)
    low_far, high_far = in_plane(low_up, 2, 1), in_plane(high_down, 2, -1)

    ring = jnp.stack([weighted, along_x(weighted, 1), along_x(weighted, -1), along_x(weighted, 2)])
    other = lax.ppermute(ring, "core", [(i, (i + 1) % nc) for i in range(nc)])
    x_at = (x - jnp.array([0, 1, -1, 2], jnp.int32)) % nx
    row_place = jnp.concatenate([x_at * nc + core, x_at * nc + (nc - 1 - core)])
    rows = stacked_rows(row_place, [ring, other])

    copies = jnp.broadcast_to(vectors[None], (ny * nz, *vectors.shape))
    column_vectors = lax.all_to_all(copies, ("y", "z"), 0, 0, tiled=True)

    def place(*offsets):
        steps = jnp.array(offsets, jnp.int32)
        along_y = (y - jnp.where(core == 0, steps[:, 0], steps[:, 1])) % ny
        along_z = (z - jnp.where(core == 0, steps[:, 1], steps[:, 0])) % nz
        return along_y * nz + along_z

    columns = ny * nz * block
    fill = functools.partial(into_tile, rows=rows, vectors=column_vectors, columns=columns)
    state = fill(place((0, 0), (1, 0), (-1, 0), (2, 0)), blocks=[low, high], state=None)
    state = fill(place((0, 1), (1, 1), (-1, -1), (2, -1)), blocks=[low_up, high_down], state=state)
    state = fill(place((-1, 1), (2, 1), (0, -1), (1, -1)), blocks=[high_up, low_down], state=state)
    _, partial, kernel = fill(
        place((0, 2), (1, 2), (-1, 2), (2, 2)), blocks=[low_far, high_far], state=state, last=True
    )

    shares = partial.astype(jnp.bfloat16).reshape(nx * nc, block, -1)
    shares = lax.all_to_all(shares, ("x", "core"), 0, 0, tiled=True)
    coupled = jnp.sum(shares.astype(jnp.float32), axis=0)
    diagonal = jnp.where(usable, energies, jnp.zeros_like(energies))
    product = coupled + diagonal[:, None] * vectors.astype(jnp.float32)
    return (kernel, product)


def solution(mesh):
    ny, nz = 4, mesh.shape["row"] // 4
    nx, nc = mesh.shape["col"] // 2, 2
    finer = Mesh(mesh.devices.reshape(ny, nz, nx, nc), MESH_AXES)
    in_specs = (P(MESH_AXES, None), P(MESH_AXES), P(), P(MESH_AXES), P(MESH_AXES, None))
    out_specs = (P(("y", "z"), ("x", "core")), P(MESH_AXES, None))
    return jax.shard_map(work, mesh=finer, in_specs=in_specs, out_specs=out_specs, check_vma=False)
```
